8 devices in a mesh: dp: 8 (over z, y, x, core).
Axes of the slice: x: 2, y: 2, z: 1, core: 2. Of those that a mesh axis runs over, the one named last changes fastest.
Arguments:
- grad_local: float32 [8, 16045056], P('dp')
- params: float32 [16045056], P('dp')
- accumulator: float32 [16045056], P('dp')
- learn_rate: float32 [], replicated
- clip_max: float32 [], replicated
Outputs:
- output 1: float32 [16045056], P('dp')
- output 2: float32 [16045056], P('dp')
- output 3: bfloat16 [16045056], replicated
- output 4: float32 [], replicated
All inputs are finite; a program needn't handle non-finite values.
Results may differ from the reference program's by a relative error of at most 0.001.
Values sent between devices are 32-bit elements.
A program may use at most 1 GiB of HBM per device.

```python
import math
import jax
import jax.numpy as jnp

DEVICES = 8
N_PARAMS = 16045056
EPS = 1e-10


def setup_inputs(seed: int = 0) -> dict:
    root_key = jax.random.key(seed)
    k_grad, k_par, k_acc, k_rate, k_clip = jax.random.split(root_key, 5)
    grad_local = jax.random.normal(k_grad, (DEVICES, N_PARAMS), jnp.float32) * math.sqrt(DEVICES)
    params = jax.random.normal(k_par, (N_PARAMS,), jnp.float32) * 0.1
    accumulator = jax.random.uniform(k_acc, (N_PARAMS,), jnp.float32, 0.05, 0.4)
    learn_rate = jnp.exp(jax.random.uniform(k_rate, (), jnp.float32, math.log(0.03), math.log(0.5)))
    clip_frac = jax.random.uniform(k_clip, (), jnp.float32, 0.3, 0.6)
    clip_max = clip_frac * math.sqrt(N_PARAMS)
    return {"grad_local": grad_local, "params": params, "accumulator": accumulator, "learn_rate": learn_rate, "clip_max": clip_max}


def reference(grad_local, params, accumulator, learn_rate, clip_max):
    mean_grad = jnp.sum(grad_local, axis=0) / DEVICES
    grad_norm = jnp.sqrt(jnp.sum(mean_grad * mean_grad))
    clip_scale = jnp.minimum(1.0, clip_max / grad_norm)
    clipped = mean_grad * clip_scale
    accum_new = accumulator + clipped * clipped
    param_new = params - learn_rate * clipped / (jnp.sqrt(accum_new) + EPS)
    return (param_new, accum_new, param_new.astype(jnp.bfloat16), grad_norm)
```

```python
import jax
import jax.numpy as jnp
from jax import lax
from jax.experimental import pallas as pl
from jax.experimental.pallas import tpu as pltpu
from jax.sharding import PartitionSpec as P

EPS = 1e-10
MESH = pl.DeviceIdType.MESH
DEVICES = 8
LANES = 128
N = 14
R = 560
BLOCK = 15669
OVER = 2 * N * R - BLOCK
SLOTS = 4
LAG = 4
GROUP = 80


def body(scal, grad, w_in, a_in, full, w_out, a_out, n_out,
         wv, av, gv, rx, ry, stage, sx, sy, acc, parts,
         wa_sem, load_sem, sendx, sendy, recvx, recvy, dsend, drecv, psend, precv,
         agsend, agd_send, agd_recv, loc_sem):
    me = lax.axis_index("dp")
    c, x, y = lax.rem(me, 2), lax.rem(me // 2, 2), me // 4

    def dev(cc, xx, yy):
        return (yy * 2 + xx) * 2 + cc

    nx, ny, nd, mate = dev(c, 1 - x, y), dev(c, x, 1 - y), dev(c, 1 - x, 1 - y), dev(1 - c, x, y)
    mx, my, md = dev(1 - c, 1 - x, y), dev(1 - c, x, 1 - y), dev(1 - c, 1 - x, 1 - y)

    def rcopy(src, dst, ssem, rsem, to):
        return pltpu.make_async_remote_copy(src, dst, ssem, rsem, device_id=(to,), device_id_type=MESH)

    barrier = pltpu.get_barrier_semaphore()
    for k in range(1, DEVICES):
        pl.semaphore_signal(barrier, inc=1, device_id=(lax.rem(me + k, DEVICES),), device_id_type=MESH)
    pl.semaphore_wait(barrier, DEVICES - 1)

    def start_row(half, i):
        if half == 0:
            return i * R
        return (N + i) * R - OVER * ((i + 1) // N)

    def d2d(blk, lo, size, k):
        rows = pl.ds(blk * BLOCK + lo, size)
        return rcopy(grad.at[rows], full.at[rows], dsend.at[k], drecv.at[k], mate)

    def d2d_first(blk, half, i, last):
        size = R - OVER if (last and half == 1) else R
        return d2d(blk, (half * N + i) * R, size, half * N + i)

    WHOLE = ((2 * N, 0), (2 * N + 1, 1), (2 * N + 2, 1), (2 * N + 3, 0), (2 * N + 4, 0), (2 * N + 5, 1))

    def d2d_whole(blks, k):
        sem, half = WHOLE[k]
        return d2d(blks[k], half * N * R, N * R - half * OVER, sem)

    theirs = (mx, my, mx, my, mate, mate)
    mine = (nx, ny, nx, ny, me, me)

    def issue(i, _):
        d2d_first(md, 0, i, False).start()
        d2d_first(md, 1, i, False).start()
        return 0

    lax.fori_loop(0, N - 1, issue, 0)
    d2d_first(md, 0, N - 1, True).start()
    d2d_first(md, 1, N - 1, True).start()
    for k in range(6):
        d2d_whole(theirs, k).start()

    def loads(items, first, i, bank):
        out = []
        for k, (blk, half) in enumerate(items):
            rows = pl.ds(blk * BLOCK + start_row(half, i), R)
            q = first + k
            out.append(pltpu.make_async_copy(grad.at[rows], stage.at[bank, q, 0], load_sem.at[bank, q, 0]))
            out.append(pltpu.make_async_copy(full.at[rows], stage.at[bank, q, 1], load_sem.at[bank, q, 1]))
        return out

    def start_all(copies):
        for cp in copies:
            cp.start()

    def wait_all(copies):
        for cp in copies:
            cp.wait()

    def sends(phase, i):
        slot = lax.rem(phase * N + i, SLOTS)
        rows = pl.ds(pl.multiple_of(i * R, 8), R)
        return (rcopy(sx.at[slot], rx.at[phase, rows], sendx.at[slot], recvx.at[phase, i], nx),
                rcopy(sy.at[slot], ry.at[phase, rows], sendy.at[slot], recvy.at[phase, i], ny))

    def free_slot(phase, i):
        def go():
            for cp in sends(phase, i):
                cp.wait_send()
        if phase == 0:
            pl.when(i >= SLOTS)(go)
        else:
            go()

    def step(phase, items, i, more):
        bank = lax.rem(i, 2)
        slot = lax.rem(phase * N + i, SLOTS)
        wait_all(loads(items, 0, i, bank))
        free_slot(phase, i)
        if phase < 2:
            sx[slot] = stage[bank, 0, 0] + stage[bank, 0, 1]
            sy[slot] = stage[bank, 1, 0] + stage[bank, 1, 1]
        else:
            cx, cy = sends(0, i)
            cx.wait_recv()
            cy.wait_recv()
            rows = pl.ds(pl.multiple_of(i * R, 8), R)
            sx[slot] = stage[bank, 0, 0] + stage[bank, 0, 1] + ry[0, rows]
            sy[slot] = stage[bank, 1, 0] + stage[bank, 1, 1] + rx[0, rows]
        start_all(sends(phase, i))
        if more is not None:
            more(i + 1)
            start_all(loads(items, 0, i + 1, lax.rem(i + 1, 2)))

    items0 = ((nd, 0), (nd, 1))

    def arrived(i, last=False):
        d2d_first(nd, 0, i, last).wait_recv()
        d2d_first(nd, 1, i, last).wait_recv()

    arrived(0)
    start_all(loads(items0, 0, 0, 0))

    def loop0(i, _):
        step(0, items0, i, arrived)
        return 0

    lax.fori_loop(0, N - 2, loop0, 0)
    step(0, items0, N - 2, lambda i: arrived(i, True))
    step(0, items0, N - 1, None)

    body_rows = (2 * N - 1) * R
    wa = []
    for k, (src, dst) in enumerate(((w_in, wv), (a_in, av))):
        wa.append(pltpu.make_async_copy(src.at[pl.ds(0, body_rows)], dst.at[pl.ds(0, body_rows)], wa_sem.at[k, 0]))
        wa.append(pltpu.make_async_copy(src.at[pl.ds(BLOCK - R, R)], dst.at[pl.ds(body_rows, R)], wa_sem.at[k, 1]))
    start_all(wa)

    items1 = ((nx, 0), (ny, 1))
    d2d_whole(mine, 0).wait_recv()
    d2d_whole(mine, 1).wait_recv()
    start_all(loads(items1, 0, 0, 0))

    def loop1(i, _):
        step(1, items1, i, lambda i: None)
        return 0

    lax.fori_loop(0, N - 1, loop1, 0)
    step(1, items1, N - 1, None)

    items2 = ((nx, 1), (ny, 0))
    itemsm = ((me, 0), (me, 1))
    for k in range(2, 6):
        d2d_whole(mine, k).wait_recv()
    start_all(loads(items2, 0, 0, 0))
    start_all(loads(itemsm, 2, 0, 0))
    acc[...] = jnp.zeros_like(acc)

    def own(j, more):
        bank = lax.rem(j, 2)
        wait_all(loads(itemsm, 2, j, bank))
        rows = pl.ds(pl.multiple_of(j * R, 8), R)
        brows = pl.ds(pl.multiple_of((N + j) * R, 8), R)
        for phase in (1, 2):
            for cp in sends(phase, j):
                cp.wait_recv()
        if more:
            start_all(loads(itemsm, 2, j + 1, lax.rem(j + 1, 2)))
        ga = (stage[bank, 2, 0] + stage[bank, 2, 1] + rx[1, rows] + ry[2, rows]) * (1.0 / DEVICES)
        gv[rows] = ga
        sq = jnp.sum((ga * ga).reshape(R // 8, 8, LANES), axis=0)
        gb = (stage[bank, 3, 0] + stage[bank, 3, 1] + ry[1, rows] + rx[2, rows]) * (1.0 / DEVICES)
        gv[brows] = gb
        skip = OVER * ((j + 1) // N)
        row = lax.broadcasted_iota(jnp.int32, (R, LANES), 0)
        gb = jnp.where(row >= skip, gb, 0.0)
        acc[...] += sq + jnp.sum((gb * gb).reshape(R // 8, 8, LANES), axis=0)

    def loop2(i, _):
        step(2, items2, i, lambda i: None)

        @pl.when(i >= LAG)
        def _():
            own(i - LAG, True)
        return 0

    lax.fori_loop(0, N - 1, loop2, 0)
    step(2, items2, N - 1, None)

    def loop3(j, _):
        own(j, True)
        return 0

    lax.fori_loop(N - 1 - LAG, N - 1, loop3, 0)
    own(N - 1, False)

    parts[me] = acc[...]

    def part(k):
        to = lax.rem(me + k, DEVICES)
        return rcopy(acc, parts.at[me], psend.at[k - 1], precv.at[k - 1], to)

    def part_in(k):
        frm = lax.rem(me + DEVICES - k, DEVICES)
        return rcopy(acc, parts.at[frm], psend.at[k - 1], precv.at[k - 1], me)

    for k in range(1, DEVICES):
        part(k).start()
    for i in range(N - SLOTS, N):
        for cp in sends(2, i):
            cp.wait_send()
    wait_all(wa)
    for k in range(1, DEVICES):
        part_in(k).wait_recv()
    total = jnp.sum(jnp.sum(parts[...], axis=0))
    norm = jnp.sqrt(jnp.full((8, LANES), total, jnp.float32))
    n_out[...] = norm
    lr = scal[0]
    scale = jnp.minimum(1.0, jnp.full((8, LANES), scal[1], jnp.float32) / norm)

    def update(chunk):
        def group(k, _):
            rows = pl.ds(pl.multiple_of(chunk * R + k * GROUP, 8), GROUP)
            shape = (GROUP // 8, 8, LANES)
            h = gv[rows].reshape(shape) * scale[None]
            a = av[rows].reshape(shape) + h * h
            w = wv[rows].reshape(shape) - lr * h / (jnp.sqrt(a) + EPS)
            av[rows] = a.reshape(GROUP, LANES)
            wv[rows] = w.reshape(GROUP, LANES)
            return 0
        lax.fori_loop(0, R // GROUP, group, 0)

    def place(half, i, last):
        cut = OVER if (last and half == 1) else 0
        size = R - cut
        return pl.ds((half * N + i) * R + cut, size), (half * N + i) * R, size

    def f_rows(blk, half, i, last):
        _, lo, size = place(half, i, last)
        return pl.ds(blk * BLOCK + lo, size)

    def direct(link, which, blk, half, i, last):
        v, _, _ = place(half, i, last)
        rows = f_rows(blk, half, i, last)
        sem = recvx if link == 0 else recvy
        return rcopy(wv.at[v], full.at[rows], agsend.at[link, which], sem.at[which, i], nx if link == 0 else ny)

    def passed(link, blk, half, i, last):
        rows = f_rows(blk, half, i, last)
        sem = recvx if link == 0 else recvy
        return rcopy(full.at[rows], full.at[rows], agsend.at[link, 1], sem.at[1, i], nx if link == 0 else ny)

    def share(src, rows, k):
        return rcopy(src, full.at[rows], agd_send.at[k], agd_recv.at[k], mate)

    def emit(i, last):
        update(i)
        direct(0, 0, me, 0, i, last).start()
        update(N + i)
        direct(1, 0, me, 1, i, last).start()
        for half in (0, 1):
            v, lo, size = place(half, i, last)
            rows = f_rows(me, half, i, last)
            share(wv.at[v], rows, 0).start()
            pltpu.make_async_copy(wv.at[v], full.at[rows], loc_sem.at[0]).start()
            pltpu.make_async_copy(wv.at[v], w_out.at[pl.ds(lo, size)], loc_sem.at[1]).start()
            pltpu.make_async_copy(av.at[v], a_out.at[pl.ds(lo, size)], loc_sem.at[2]).start()

    def each(fn):
        def loop(i, _):
            fn(i, False)
            return 0
        lax.fori_loop(0, N - 1, loop, 0)
        fn(N - 1, True)

    each(emit)

    def forward(i, last):
        direct(0, 0, nx, 0, i, last).wait_recv()
        rows = f_rows(nx, 0, i, last)
        passed(1, nx, 0, i, last).start()
        share(full.at[rows], rows, 1).start()
        direct(1, 0, ny, 1, i, last).wait_recv()
        rows = f_rows(ny, 1, i, last)
        passed(0, ny, 1, i, last).start()
        share(full.at[rows], rows, 2).start()

    each(forward)

    def second(i, last):
        direct(0, 2, me, 1, i, last).start()
        direct(1, 2, me, 0, i, last).start()

    each(second)

    def take_passed(i, last):
        passed(1, nd, 0, i, last).wait_recv()
        rows = f_rows(nd, 0, i, last)
        share(full.at[rows], rows, 3).start()
        passed(0, nd, 1, i, last).wait_recv()
        rows = f_rows(nd, 1, i, last)
        share(full.at[rows], rows, 3).start()

    each(take_passed)

    def take_second(i, last):
        direct(0, 2, nx, 1, i, last).wait_recv()
        rows = f_rows(nx, 1, i, last)
        share(full.at[rows], rows, 1).start()
        direct(1, 2, ny, 0, i, last).wait_recv()
        rows = f_rows(ny, 0, i, last)
        share(full.at[rows], rows, 2).start()

    each(take_second)

    def d2d_out(i, last):
        d2d_first(md, 0, i, last).wait_send()
        d2d_first(md, 1, i, last).wait_send()

    each(d2d_out)
    for k in range(6):
        d2d_whole(theirs, k).wait_send()
    for k in range(1, DEVICES):
        part(k).wait_send()
    for link, halves in ((0, (0, 1, 1)), (1, (1, 0, 0))):
        for which, half in enumerate(halves):
            rows = pl.ds(0, N * R - half * OVER)
            rcopy(full.at[rows], full.at[rows], agsend.at[link, which], recvx.at[0, 0], mate).wait_send()
    whole = pl.ds(0, BLOCK)
    for k in range(3):
        pltpu.make_async_copy(full.at[whole], full.at[whole], loc_sem.at[k]).wait()
    for k in range(4):
        cp = rcopy(full.at[whole], full.at[whole], agd_send.at[k], agd_recv.at[k], mate)
        cp.wait_send()
        cp.wait_recv()


def solution(mesh):
    def local_step(grad_row, param_blk, accum_blk, learn_rate, clip_max):
        rows = grad_row.shape[1] // LANES
        f32 = jnp.float32
        any_spec = pl.BlockSpec(memory_space=pl.ANY)
        dma = pltpu.SemaphoreType.DMA
        full, w_new, a_new, norm = pl.pallas_call(
            body,
            name="adagrad_exchange",
            out_shape=(
                jax.ShapeDtypeStruct((rows, LANES), f32),
                jax.ShapeDtypeStruct((BLOCK, LANES), f32),
                jax.ShapeDtypeStruct((BLOCK, LANES), f32),
                jax.ShapeDtypeStruct((8, LANES), f32),
            ),
            in_specs=[pl.BlockSpec(memory_space=pltpu.SMEM), any_spec, any_spec, any_spec],
            out_specs=(any_spec, any_spec, any_spec, pl.BlockSpec(memory_space=pltpu.VMEM)),
            scratch_shapes=[
                pltpu.VMEM((2 * N * R, LANES), f32),
                pltpu.VMEM((2 * N * R, LANES), f32),
                pltpu.VMEM((2 * N * R, LANES), f32),
                pltpu.VMEM((3, N * R, LANES), f32),
                pltpu.VMEM((3, N * R, LANES), f32),
                pltpu.VMEM((2, 4, 2, R, LANES), f32),
                pltpu.VMEM((SLOTS, R, LANES), f32),
                pltpu.VMEM((SLOTS, R, LANES), f32),
                pltpu.VMEM((8, LANES), f32),
                pltpu.VMEM((DEVICES, 8, LANES), f32),
                dma((2, 2)), dma((2, 4, 2)), dma((SLOTS,)), dma((SLOTS,)),
                dma((3, N)), dma((3, N)), dma((2 * N + 6,)), dma((2 * N + 6,)),
                dma((DEVICES - 1,)), dma((DEVICES - 1,)),
                dma((2, 3)), dma((4,)), dma((4,)), dma((3,)),
            ],
            compiler_params=pltpu.CompilerParams(
                collective_id=0, has_side_effects=True, vmem_limit_bytes=64_000_000
            ),
        )(
            jnp.stack([learn_rate, clip_max]),
            grad_row.reshape(rows, LANES),
            param_blk.reshape(BLOCK, LANES),
            accum_blk.reshape(BLOCK, LANES),
        )
        return w_new.reshape(-1), a_new.reshape(-1), full.astype(jnp.bfloat16).reshape(-1), norm[0, 0]

    return jax.shard_map(
        local_step, mesh=mesh,
        in_specs=(P("dp", None), P("dp"), P("dp"), P(), P()),
        out_specs=(P("dp"), P("dp"), P(), P()), check_vma=False,
    )
```

```python
import jax
import jax.numpy as jnp
from jax import lax
from jax.experimental import pallas as pl
from jax.experimental.pallas import tpu as pltpu
from jax.sharding import PartitionSpec as P


EPS = 1e-10
MESH = pl.DeviceIdType.MESH
DEVICES = 8
LANES = 128
N = 14
R = 560
BLOCK = 15669
OVER = 2 * N * R - BLOCK
SLOTS = 4
LAG = 4
GROUP = 80
PIECES = (3360, 1680, 560)
LATE = sum(PIECES) // R
BULK_ROWS = 3968
MARGIN = 16


def body(lr_in, clip_in, grad, w_in, a_in, full, w_out, a_out, n_out, *rest):
    late_x, late_y = rest[: len(PIECES)], rest[len(PIECES) : 2 * len(PIECES)]
    exchange(lr_in, clip_in, grad, w_in, a_in, full, w_out, a_out, n_out, late_x, late_y, *rest[2 * len(PIECES) :])


def piece_rows():
    lo = 0
    for size in PIECES:
        yield N * R + lo, (N - LATE) * R + lo, size
        lo += size


def exchange(lr_in, clip_in, grad, w_in, a_in, full, w_out, a_out, n_out, late_x, late_y,
         wv, av, gv, rx, ry, stage, sx, sy, acc, parts,
         wa_sem, load_sem, sendx, sendy, recvx, recvy, dsend, drecv, psend, precv,
         agsend, agd_send, agd_recv, loc_sem, late_sem):
    me = lax.axis_index("dp")
    c, x, y = lax.rem(me, 2), lax.rem(me // 2, 2), me // 4

    def dev(cc, xx, yy):
        return (yy * 2 + xx) * 2 + cc

    nx, ny, nd, mate = dev(c, 1 - x, y), dev(c, x, 1 - y), dev(c, 1 - x, 1 - y), dev(1 - c, x, y)
    mx, my, md = dev(1 - c, 1 - x, y), dev(1 - c, x, 1 - y), dev(1 - c, 1 - x, 1 - y)

    def rcopy(src, dst, ssem, rsem, to):
        return pltpu.make_async_remote_copy(src, dst, ssem, rsem, device_id=(to,), device_id_type=MESH)

    barrier = pltpu.get_barrier_semaphore()
    for k in range(1, DEVICES):
        pl.semaphore_signal(barrier, inc=1, device_id=(lax.rem(me + k, DEVICES),), device_id_type=MESH)
    pl.semaphore_wait(barrier, DEVICES - 1)

    def start_row(half, i):
        if half == 0:
            return i * R
        return (N + i) * R - OVER * ((i + 1) // N)

    def d2d(blk, lo, size, k):
        rows = pl.ds(blk * BLOCK + lo, size)
        return rcopy(grad.at[rows], full.at[rows], dsend.at[k], drecv.at[k], mate)

    def d2d_first(blk, half, i, last):
        size = R - OVER if (last and half == 1) else R
        return d2d(blk, (half * N + i) * R, size, half * N + i)

    WHOLE = ((2 * N, 0), (2 * N + 1, 1), (2 * N + 2, 1), (2 * N + 3, 0), (2 * N + 4, 0), (2 * N + 5, 1))

    def d2d_whole(blks, k):
        sem, half = WHOLE[k]
        return d2d(blks[k], half * N * R, N * R - half * OVER, sem)

    theirs = (mx, my, mx, my, mate, mate)
    mine = (nx, ny, nx, ny, me, me)

    def issue(i, _):
        d2d_first(md, 0, i, False).start()
        d2d_first(md, 1, i, False).start()
        return 0

    lax.fori_loop(0, N - 1, issue, 0)
    d2d_first(md, 0, N - 1, True).start()
    d2d_first(md, 1, N - 1, True).start()
    for k in range(6):
        d2d_whole(theirs, k).start()

    def loads(items, first, i, bank):
        out = []
        for k, (blk, half) in enumerate(items):
            rows = pl.ds(blk * BLOCK + start_row(half, i), R)
            q = first + k
            out.append(pltpu.make_async_copy(grad.at[rows], stage.at[bank, q, 0], load_sem.at[bank, q, 0]))
            out.append(pltpu.make_async_copy(full.at[rows], stage.at[bank, q, 1], load_sem.at[bank, q, 1]))
        return out

    def start_all(copies):
        for cp in copies:
            cp.start()

    def wait_all(copies):
        for cp in copies:
            cp.wait()

    def sends(phase, i):
        slot = lax.rem(phase * N + i, SLOTS)
        rows = pl.ds(pl.multiple_of(i * R, 8), R)
        return (rcopy(sx.at[slot], rx.at[phase, rows], sendx.at[slot], recvx.at[phase, i], nx),
                rcopy(sy.at[slot], ry.at[phase, rows], sendy.at[slot], recvy.at[phase, i], ny))

    def free_slot(phase, i):
        def go():
            for cp in sends(phase, i):
                cp.wait_send()

        if phase == 0:
            pl.when(i >= SLOTS)(go)
        else:
            go()

    def step(phase, items, i, more):
        bank = lax.rem(i, 2)
        slot = lax.rem(phase * N + i, SLOTS)
        wait_all(loads(items, 0, i, bank))
        free_slot(phase, i)
        if phase < 2:
            sx[slot] = stage[bank, 0, 0] + stage[bank, 0, 1]
            sy[slot] = stage[bank, 1, 0] + stage[bank, 1, 1]
        else:
            cx, cy = sends(0, i)
            cx.wait_recv()
            cy.wait_recv()
            rows = pl.ds(pl.multiple_of(i * R, 8), R)
            sx[slot] = stage[bank, 0, 0] + stage[bank, 0, 1] + ry[0, rows]
            sy[slot] = stage[bank, 1, 0] + stage[bank, 1, 1] + rx[0, rows]
        start_all(sends(phase, i))
        if more is not None:
            more(i + 1)
            start_all(loads(items, 0, i + 1, lax.rem(i + 1, 2)))

    items0 = ((nd, 0), (nd, 1))

    def arrived(i, last=False):
        d2d_first(nd, 0, i, last).wait_recv()
        d2d_first(nd, 1, i, last).wait_recv()

    arrived(0)
    start_all(loads(items0, 0, 0, 0))

    def loop0(i, _):
        step(0, items0, i, arrived)
        return 0

    lax.fori_loop(0, N - 2, loop0, 0)
    step(0, items0, N - 2, lambda i: arrived(i, True))
    step(0, items0, N - 1, None)

    body_rows = (2 * N - 1) * R
    wa = []
    for k, (src, dst) in enumerate(((w_in, wv), (a_in, av))):
        wa.append(pltpu.make_async_copy(src.at[pl.ds(0, body_rows)], dst.at[pl.ds(0, body_rows)], wa_sem.at[k, 0]))
        wa.append(pltpu.make_async_copy(src.at[pl.ds(BLOCK - R, R)], dst.at[pl.ds(body_rows, R)], wa_sem.at[k, 1]))
    start_all(wa)

    items1 = ((nx, 0), (ny, 1))
    d2d_whole(mine, 0).wait_recv()
    d2d_whole(mine, 1).wait_recv()
    start_all(loads(items1, 0, 0, 0))

    def loop1(i, _):
        step(1, items1, i, lambda i: None)
        return 0

    lax.fori_loop(0, N - 1, loop1, 0)
    step(1, items1, N - 1, None)

    items2 = ((nx, 1), (ny, 0))
    itemsm = ((me, 0), (me, 1))
    for k in range(2, 6):
        d2d_whole(mine, k).wait_recv()
    start_all(loads(items2, 0, 0, 0))
    start_all(loads(itemsm, 2, 0, 0))
    acc[...] = jnp.zeros_like(acc)

    def own(j, more):
        bank = lax.rem(j, 2)
        wait_all(loads(itemsm, 2, j, bank))
        rows = pl.ds(pl.multiple_of(j * R, 8), R)
        brows = pl.ds(pl.multiple_of((N + j) * R, 8), R)
        for phase in (1, 2):
            for cp in sends(phase, j):
                cp.wait_recv()
        if more:
            start_all(loads(itemsm, 2, j + 1, lax.rem(j + 1, 2)))
        ga = (stage[bank, 2, 0] + stage[bank, 2, 1] + rx[1, rows] + ry[2, rows]) * (1.0 / DEVICES)
        gv[rows] = ga
        sq = jnp.sum((ga * ga).reshape(R // 8, 8, LANES), axis=0)
        gb = (stage[bank, 3, 0] + stage[bank, 3, 1] + ry[1, rows] + rx[2, rows]) * (1.0 / DEVICES)
        gv[brows] = gb
        skip = OVER * ((j + 1) // N)
        row = lax.broadcasted_iota(jnp.int32, (R, LANES), 0)
        gb = jnp.where(row >= skip, gb, 0.0)
        acc[...] += sq + jnp.sum((gb * gb).reshape(R // 8, 8, LANES), axis=0)

    def loop2(i, _):
        step(2, items2, i, lambda i: None)

        @pl.when(i >= LAG)
        def _():
            own(i - LAG, True)

        return 0

    lax.fori_loop(0, N - 1, loop2, 0)
    step(2, items2, N - 1, None)

    def loop3(j, _):
        own(j, True)
        return 0

    lax.fori_loop(N - 1 - LAG, N - 1, loop3, 0)
    own(N - 1, False)

    parts[me] = acc[...]

    def part(k):
        to = lax.rem(me + k, DEVICES)
        return rcopy(acc, parts.at[me], psend.at[k - 1], precv.at[k - 1], to)

    def part_in(k):
        frm = lax.rem(me + DEVICES - k, DEVICES)
        return rcopy(acc, parts.at[frm], psend.at[k - 1], precv.at[k - 1], me)

    for k in range(1, DEVICES):
        part(k).start()
    for i in range(N - SLOTS, N):
        for cp in sends(2, i):
            cp.wait_send()
    wait_all(wa)
    for k in range(1, DEVICES):
        part_in(k).wait_recv()
    total = jnp.sum(jnp.sum(parts[...], axis=0))
    norm = jnp.sqrt(jnp.full((8, LANES), total, jnp.float32))
    n_out[...] = norm
    lr = lr_in[0]
    scale = jnp.minimum(1.0, jnp.full((8, LANES), clip_in[0], jnp.float32) / norm)

    def update(chunk):
        def group(k, _):
            rows = pl.ds(pl.multiple_of(chunk * R + k * GROUP, 8), GROUP)
            shape = (GROUP // 8, 8, LANES)
            h = gv[rows].reshape(shape) * scale[None]
            a = av[rows].reshape(shape) + h * h
            w = wv[rows].reshape(shape) - lr * h / (jnp.sqrt(a) + EPS)
            av[rows] = a.reshape(GROUP, LANES)
            wv[rows] = w.reshape(GROUP, LANES)
            return 0

        lax.fori_loop(0, R // GROUP, group, 0)

    def place(half, i, last):
        cut = OVER if (last and half == 1) else 0
        size = R - cut
        return pl.ds((half * N + i) * R + cut, size), (half * N + i) * R, size

    def f_rows(blk, half, i, last):
        _, lo, size = place(half, i, last)
        return pl.ds(blk * BLOCK + lo, size)

    def direct(link, which, blk, half, i, last):
        v, _, _ = place(half, i, last)
        rows = f_rows(blk, half, i, last)
        sem = recvx if link == 0 else recvy
        return rcopy(wv.at[v], full.at[rows], agsend.at[link, which], sem.at[which, i], nx if link == 0 else ny)

    def passed(link, blk, half, i, last):
        rows = f_rows(blk, half, i, last)
        sem = recvx if link == 0 else recvy
        return rcopy(full.at[rows], full.at[rows], agsend.at[link, 1], sem.at[1, i], nx if link == 0 else ny)

    def share(src, rows, k):
        return rcopy(src, full.at[rows], agd_send.at[k], agd_recv.at[k], mate)

    def emit(i, last):
        update(i)
        direct(0, 0, me, 0, i, last).start()
        update(N + i)
        direct(1, 0, me, 1, i, last).start()
        for half in (0, 1):
            v, lo, size = place(half, i, last)
            rows = f_rows(me, half, i, last)
            share(wv.at[v], rows, 0).start()
            pltpu.make_async_copy(wv.at[v], full.at[rows], loc_sem.at[0]).start()
            pltpu.make_async_copy(wv.at[v], w_out.at[pl.ds(lo, size)], loc_sem.at[1]).start()
            pltpu.make_async_copy(av.at[v], a_out.at[pl.ds(lo, size)], loc_sem.at[2]).start()

    def each(fn):
        def loop(i, _):
            fn(i, False)
            return 0

        lax.fori_loop(0, N - 1, loop, 0)
        fn(N - 1, True)

    each(emit)
    late = []
    for k, (row_x, row_y, size) in enumerate(piece_rows()):
        for q, (dst, row) in enumerate(((late_x[k], row_x), (late_y[k], row_y))):
            rows = pl.ds(row - MARGIN, size + 2 * MARGIN)
            late.append(pltpu.make_async_copy(wv.at[rows], dst, late_sem.at[k, q]))
    start_all(late)

    def forward(i, last):
        direct(0, 0, nx, 0, i, last).wait_recv()
        rows = f_rows(nx, 0, i, last)
        passed(1, nx, 0, i, last).start()
        share(full.at[rows], rows, 1).start()
        direct(1, 0, ny, 1, i, last).wait_recv()
        rows = f_rows(ny, 1, i, last)
        passed(0, ny, 1, i, last).start()
        share(full.at[rows], rows, 2).start()

    each(forward)

    def loop4(i, _):
        direct(0, 2, me, 1, i, False).start()
        direct(1, 2, me, 0, i - LATE, False).start()
        return 0

    lax.fori_loop(LATE, N - 1, loop4, 0)
    direct(0, 2, me, 1, N - 1, True).start()
    direct(1, 2, me, 0, N - 1 - LATE, False).start()

    def take_passed(i, last):
        passed(1, nd, 0, i, last).wait_recv()
        rows = f_rows(nd, 0, i, last)
        share(full.at[rows], rows, 3).start()
        passed(0, nd, 1, i, last).wait_recv()
        rows = f_rows(nd, 1, i, last)
        share(full.at[rows], rows, 3).start()

    each(take_passed)

    def take_second(i, last):
        direct(0, 2, nx, 1, i, last).wait_recv()
        rows = f_rows(nx, 1, i, last)
        share(full.at[rows], rows, 1).start()
        direct(1, 2, ny, 0, i - LATE, False).wait_recv()
        rows = f_rows(ny, 0, i - LATE, False)
        share(full.at[rows], rows, 2).start()

    def loop5(i, _):
        take_second(i, False)
        return 0

    lax.fori_loop(LATE, N - 1, loop5, 0)
    take_second(N - 1, True)

    def d2d_out(i, last):
        d2d_first(md, 0, i, last).wait_send()
        d2d_first(md, 1, i, last).wait_send()

    each(d2d_out)
    for k in range(6):
        d2d_whole(theirs, k).wait_send()
    for k in range(1, DEVICES):
        part(k).wait_send()
    for link, halves in ((0, (0, 1, 1)), (1, (1, 0, 0))):
        for which, half in enumerate(halves):
            rows = pl.ds(0, N * R - half * OVER - (LATE * R if which == 2 else 0))
            rcopy(full.at[rows], full.at[rows], agsend.at[link, which], recvx.at[0, 0], mate).wait_send()
    whole = pl.ds(0, BLOCK)
    for k in range(3):
        pltpu.make_async_copy(full.at[whole], full.at[whole], loc_sem.at[k]).wait()
    wait_all(late)
    for k in range(4):
        rows = pl.ds(0, BLOCK - (LATE * R if k in (1, 2) else 0))
        cp = rcopy(full.at[rows], full.at[rows], agd_send.at[k], agd_recv.at[k], mate)
        cp.wait_send()
        cp.wait_recv()


def bulk_body(f_ref, w_ref, a_ref, copy_ref, w_out, a_out):
    copy_ref[...] = f_ref[...].astype(jnp.bfloat16)
    w_out[...] = w_ref[...]
    a_out[...] = a_ref[...]


def bulk(full, w_new, a_new):
    big, small = (BULK_ROWS, LANES), (BULK_ROWS // 8 + 8 - BULK_ROWS // 8 % 8, LANES)
    at = lambda i: (i, 0)
    specs = [pl.BlockSpec(big, at), pl.BlockSpec(small, at), pl.BlockSpec(small, at)]
    return pl.pallas_call(
        bulk_body,
        name="bulk",
        grid=(pl.cdiv(full.shape[0], BULK_ROWS),),
        out_shape=(
            jax.ShapeDtypeStruct(full.shape, jnp.bfloat16),
            jax.ShapeDtypeStruct(w_new.shape, w_new.dtype),
            jax.ShapeDtypeStruct(a_new.shape, a_new.dtype),
        ),
        in_specs=specs,
        out_specs=tuple(specs),
        compiler_params=pltpu.CompilerParams(vmem_limit_bytes=54_000_000),
        cost_estimate=pl.CostEstimate(flops=full.size, bytes_accessed=8 * full.size, transcendentals=0),
    )(full, w_new, a_new)


def place_pieces(k, size):
    rows = size + MARGIN

    def kernel(_, px, py, mx_, my_, out, f32s, b16s, in_sem, out_sem):
        me = lax.axis_index("dp")
        c, x, y = lax.rem(me, 2), lax.rem(me // 2, 2), me // 4
        starts = list(piece_rows())[k]
        ins, outs = [], []
        for q, (src, cc, xx, yy, lo) in enumerate((
            (px, c, 1 - x, y, starts[0]), (py, c, x, 1 - y, starts[1]),
            (mx_, 1 - c, 1 - x, y, starts[0]), (my_, 1 - c, x, 1 - y, starts[1]),
        )):
            first = ((yy * 2 + xx) * 2 + cc) * BLOCK + lo
            shift = lax.rem(first, MARGIN)
            ins.append(pltpu.make_async_copy(src.at[pl.ds(MARGIN - shift, rows)], f32s.at[q], in_sem.at[q]))
            aligned = pl.multiple_of(first - shift, MARGIN)
            outs.append(pltpu.make_async_copy(b16s.at[q], out.at[pl.ds(aligned, rows)], out_sem.at[q]))
        for cp in ins:
            cp.start()
        for q in range(4):
            ins[q].wait()
            b16s[q] = f32s[q].astype(jnp.bfloat16)
            outs[q].start()
        for cp in outs:
            cp.wait()

    any_spec = pl.BlockSpec(memory_space=pl.ANY)

    def call(out, px, py, mx_, my_):
        return pl.pallas_call(
            kernel,
            out_shape=jax.ShapeDtypeStruct(out.shape, out.dtype),
            in_specs=[any_spec] * 5,
            out_specs=any_spec,
            input_output_aliases={0: 0},
            scratch_shapes=[
                pltpu.VMEM((4, rows, LANES), jnp.float32),
                pltpu.VMEM((4, rows, LANES), jnp.bfloat16),
                pltpu.SemaphoreType.DMA((4,)),
                pltpu.SemaphoreType.DMA((4,)),
            ],
            compiler_params=pltpu.CompilerParams(vmem_limit_bytes=32_000_000),
            cost_estimate=pl.CostEstimate(flops=10_000_000, bytes_accessed=6 * 4 * rows * LANES, transcendentals=0),
        )(out, px, py, mx_, my_)

    return call


def solution(mesh):
    def local_step(grad_row, param_blk, accum_blk, learn_rate, clip_max):
        rows = grad_row.shape[1] // LANES
        f32 = jnp.float32
        any_spec = pl.BlockSpec(memory_space=pl.ANY)
        dma = pltpu.SemaphoreType.DMA
        smem = pl.BlockSpec(memory_space=pltpu.SMEM)
        late = tuple(jax.ShapeDtypeStruct((size + 2 * MARGIN, LANES), f32) for size in PIECES)
        full, w_new, a_new, norm, *late = pl.pallas_call(
            body,
            name="adagrad_exchange",
            out_shape=(
                jax.ShapeDtypeStruct((rows, LANES), f32),
                jax.ShapeDtypeStruct((BLOCK, LANES), f32),
                jax.ShapeDtypeStruct((BLOCK, LANES), f32),
                jax.ShapeDtypeStruct((8, LANES), f32),
            ) + late + late,
            in_specs=[smem, smem, any_spec, any_spec, any_spec],
            out_specs=(any_spec, any_spec, any_spec, pl.BlockSpec(memory_space=pltpu.VMEM))
            + (any_spec,) * (2 * len(PIECES)),
            scratch_shapes=[
                pltpu.VMEM((2 * N * R, LANES), f32),
                pltpu.VMEM((2 * N * R, LANES), f32),
                pltpu.VMEM((2 * N * R, LANES), f32),
                pltpu.VMEM((3, N * R, LANES), f32),
                pltpu.VMEM((3, N * R, LANES), f32),
                pltpu.VMEM((2, 4, 2, R, LANES), f32),
                pltpu.VMEM((SLOTS, R, LANES), f32),
                pltpu.VMEM((SLOTS, R, LANES), f32),
                pltpu.VMEM((8, LANES), f32),
                pltpu.VMEM((DEVICES, 8, LANES), f32),
                dma((2, 2)), dma((2, 4, 2)), dma((SLOTS,)), dma((SLOTS,)),
                dma((3, N)), dma((3, N)), dma((2 * N + 6,)), dma((2 * N + 6,)),
                dma((DEVICES - 1,)), dma((DEVICES - 1,)),
                dma((2, 3)), dma((4,)), dma((4,)), dma((3,)), dma((len(PIECES), 2)),
            ],
            compiler_params=pltpu.CompilerParams(
                collective_id=0, has_side_effects=True, vmem_limit_bytes=64_000_000
            ),
        )(
            learn_rate.reshape(1),
            clip_max.reshape(1),
            grad_row.reshape(rows, LANES),
            param_blk.reshape(BLOCK, LANES),
            accum_blk.reshape(BLOCK, LANES),
        )

        def permute(v, bit):
            return lax.ppermute(v, "dp", [(k, k ^ bit) for k in range(DEVICES)])

        copy, w_new, a_new = bulk(full, w_new, a_new)
        for k, size in enumerate(PIECES):
            px = permute(late[k], 2)
            py = permute(late[len(PIECES) + k], 4)
            dx = permute(px, 1)
            dy = permute(py, 1)
            copy = place_pieces(k, size)(copy, px, py, dx, dy)
        return w_new.reshape(-1), a_new.reshape(-1), copy.reshape(-1), norm[0, 0]

    return jax.shard_map(
        local_step, mesh=mesh,
        in_specs=(P("dp", None), P("dp"), P("dp"), P(), P()),
        out_specs=(P("dp"), P("dp"), P(), P()), check_vma=False,
    )
```

```python
import jax
import jax.numpy as jnp
from jax import lax
from jax.experimental import pallas as pl
from jax.experimental.pallas import tpu as pltpu
from jax.sharding import PartitionSpec as P


EPS = 1e-10
MESH = pl.DeviceIdType.MESH
DEVICES = 8
LANES = 128
N = 14
R = 560
BLOCK = 15669
OVER = 2 * N * R - BLOCK
SLOTS = 4
LAG = 4
GROUP = 80
PIECES = (3920, 1680, 560)
LATE = sum(PIECES) // R
BULK_ROWS = 3968
MARGIN = 8


def body(lr_in, clip_in, grad, w_in, a_in, full, w_out, a_out, n_out, *rest):
    k = len(PIECES)
    exchange(lr_in, clip_in, grad, w_in, a_in, full, w_out, a_out, n_out, rest[:k], rest[k : 2 * k], *rest[2 * k :])


def piece_rows():
    yield (N + LATE) * R, (N - 1 - LATE) * R, R
    lo = 0
    for size in PIECES:
        yield N * R + lo, (N - LATE) * R + lo, size
        lo += size


def exchange(lr_in, clip_in, grad, w_in, a_in, full, w_out, a_out, n_out, late_x, late_y, tail_x, tail_y,
         wv, av, gv, rx, ry, stage, sx, sy, acc, parts,
         wa_sem, load_sem, sendx, sendy, recvx, recvy, dsend, drecv, psend, precv,
         agsend, agd_send, agd_recv, loc_sem, late_sem, tail_sem, nv, norm_sem):
    me = lax.axis_index("dp")
    c, x, y = lax.rem(me, 2), lax.rem(me // 2, 2), me // 4

    def dev(cc, xx, yy):
        return (yy * 2 + xx) * 2 + cc

    nx, ny, nd, mate = dev(c, 1 - x, y), dev(c, x, 1 - y), dev(c, 1 - x, 1 - y), dev(1 - c, x, y)
    mx, my, md = dev(1 - c, 1 - x, y), dev(1 - c, x, 1 - y), dev(1 - c, 1 - x, 1 - y)

    def rcopy(src, dst, ssem, rsem, to):
        return pltpu.make_async_remote_copy(src, dst, ssem, rsem, device_id=(to,), device_id_type=MESH)

    def own_first(half):
        rows = pl.ds(nd * BLOCK + half * N * R, R)
        return pltpu.make_async_copy(grad.at[rows], stage.at[0, half, 0], load_sem.at[0, half, 0])

    own_first(0).start()
    own_first(1).start()
    barrier = pltpu.get_barrier_semaphore()
    for k in range(1, DEVICES):
        pl.semaphore_signal(barrier, inc=1, device_id=(lax.rem(me + k, DEVICES),), device_id_type=MESH)
    pl.semaphore_wait(barrier, DEVICES - 1)

    def start_row(half, i):
        if half == 0:
            return i * R
        return (N + i) * R - OVER * ((i + 1) // N)

    def d2d(blk, lo, size, k):
        rows = pl.ds(blk * BLOCK + lo, size)
        return rcopy(grad.at[rows], full.at[rows], dsend, drecv.at[k], mate)

    def d2d_head(blk, half):
        rows = pl.ds(blk * BLOCK + half * N * R, R)
        return rcopy(grad.at[rows], stage.at[0, half, 1], dsend, drecv.at[half * N], mate)

    def d2d_first(blk, half, i, last):
        size = R - OVER if (last and half == 1) else R
        return d2d(blk, (half * N + i) * R, size, half * N + i)

    WHOLE = ((2 * N, 0), (2 * N + 1, 1), (2 * N + 2, 1), (2 * N + 3, 0), (2 * N + 4, 0), (2 * N + 5, 1))

    def d2d_whole(blks, k):
        sem, half = WHOLE[k]
        return d2d(blks[k], half * N * R, N * R - half * OVER, sem)

    theirs = (mx, my, mx, my, mate, mate)
    mine = (nx, ny, nx, ny, me, me)

    def issue(i, _):
        d2d_first(md, 0, i, False).start()
        d2d_first(md, 1, i, False).start()
        return 0

    d2d_head(md, 0).start()
    d2d_head(md, 1).start()
    lax.fori_loop(1, N - 1, issue, 0)
    d2d_first(md, 0, N - 1, True).start()
    d2d_first(md, 1, N - 1, True).start()
    for k in range(6):
        d2d_whole(theirs, k).start()

    def loads(items, first, i, bank):
        out = []
        for k, (blk, half) in enumerate(items):
            rows = pl.ds(blk * BLOCK + start_row(half, i), R)
            q = first + k
            out.append(pltpu.make_async_copy(grad.at[rows], stage.at[bank, q, 0], load_sem.at[bank, q, 0]))
            out.append(pltpu.make_async_copy(full.at[rows], stage.at[bank, q, 1], load_sem.at[bank, q, 1]))
        return out

    def start_all(copies):
        for cp in copies:
            cp.start()

    def wait_all(copies):
        for cp in copies:
            cp.wait()

    def sends(phase, i):
        slot = lax.rem(phase * N + i, SLOTS)
        rows = pl.ds(pl.multiple_of(i * R, 8), R)
        return (rcopy(sx.at[slot], rx.at[phase, rows], sendx.at[slot], recvx.at[phase, i], nx),
                rcopy(sy.at[slot], ry.at[phase, rows], sendy.at[slot], recvy.at[phase, i], ny))

    def free_slot(phase, i):
        def go():
            for cp in sends(phase, i):
                cp.wait_send()

        if phase == 0:
            pl.when(i >= SLOTS)(go)
        else:
            go()

    def step(phase, items, i, more):
        bank = lax.rem(i, 2)
        slot = lax.rem(phase * N + i, SLOTS)
        wait_all(loads(items, 0, i, bank))
        free_slot(phase, i)
        if phase < 2:
            sx[slot] = stage[bank, 0, 0] + stage[bank, 0, 1]
            sy[slot] = stage[bank, 1, 0] + stage[bank, 1, 1]
        else:
            cx, cy = sends(0, i)
            cx.wait_recv()
            cy.wait_recv()
            rows = pl.ds(pl.multiple_of(i * R, 8), R)
            sx[slot] = stage[bank, 0, 0] + stage[bank, 0, 1] + ry[0, rows]
            sy[slot] = stage[bank, 1, 0] + stage[bank, 1, 1] + rx[0, rows]
        start_all(sends(phase, i))
        if more is not None:
            more(i + 1)
            start_all(loads(items, 0, i + 1, lax.rem(i + 1, 2)))

    items0 = ((nd, 0), (nd, 1))

    def arrived(i, last=False):
        d2d_first(nd, 0, i, last).wait_recv()
        d2d_first(nd, 1, i, last).wait_recv()

    head = sends(0, 0)
    for half, slots in ((0, sx), (1, sy)):
        own_first(half).wait()
        d2d_head(nd, half).wait_recv()
        slots[0] = stage[0, half, 0] + stage[0, half, 1]
        head[half].start()
    arrived(1)
    start_all(loads(items0, 0, 1, 1))

    def loop0(i, _):
        step(0, items0, i, arrived)
        return 0

    lax.fori_loop(1, N - 2, loop0, 0)
    step(0, items0, N - 2, lambda i: arrived(i, True))
    step(0, items0, N - 1, None)

    body_rows = (2 * N - 1) * R
    wa = []
    for k, (src, dst) in enumerate(((w_in, wv), (a_in, av))):
        wa.append(pltpu.make_async_copy(src.at[pl.ds(0, body_rows)], dst.at[pl.ds(0, body_rows)], wa_sem.at[k, 0]))
        wa.append(pltpu.make_async_copy(src.at[pl.ds(BLOCK - R, R)], dst.at[pl.ds(body_rows, R)], wa_sem.at[k, 1]))
    start_all(wa)

    items1 = ((nx, 0), (ny, 1))
    d2d_whole(mine, 0).wait_recv()
    d2d_whole(mine, 1).wait_recv()
    start_all(loads(items1, 0, 0, 0))

    def loop1(i, _):
        step(1, items1, i, lambda i: None)
        return 0

    lax.fori_loop(0, N - 1, loop1, 0)
    step(1, items1, N - 1, None)

    items2 = ((nx, 1), (ny, 0))
    itemsm = ((me, 0), (me, 1))
    for k in range(2, 6):
        d2d_whole(mine, k).wait_recv()
    start_all(loads(items2, 0, 0, 0))
    start_all(loads(itemsm, 2, 0, 0))
    acc[...] = jnp.zeros_like(acc)

    def own(j, more):
        bank = lax.rem(j, 2)
        wait_all(loads(itemsm, 2, j, bank))
        rows = pl.ds(pl.multiple_of(j * R, 8), R)
        brows = pl.ds(pl.multiple_of((N + j) * R, 8), R)
        for phase in (1, 2):
            for cp in sends(phase, j):
                cp.wait_recv()
        if more:
            start_all(loads(itemsm, 2, j + 1, lax.rem(j + 1, 2)))
        ga = (stage[bank, 2, 0] + stage[bank, 2, 1] + rx[1, rows] + ry[2, rows]) * (1.0 / DEVICES)
        gv[rows] = ga
        sq = jnp.sum((ga * ga).reshape(R // 8, 8, LANES), axis=0)
        gb = (stage[bank, 3, 0] + stage[bank, 3, 1] + ry[1, rows] + rx[2, rows]) * (1.0 / DEVICES)
        gv[brows] = gb
        skip = OVER * ((j + 1) // N)
        row = lax.broadcasted_iota(jnp.int32, (R, LANES), 0)
        gb = jnp.where(row >= skip, gb, 0.0)
        acc[...] += sq + jnp.sum((gb * gb).reshape(R // 8, 8, LANES), axis=0)

    def loop2(i, _):
        step(2, items2, i, lambda i: None)

        @pl.when(i >= LAG)
        def _():
            own(i - LAG, True)

        return 0

    lax.fori_loop(0, N - 1, loop2, 0)
    step(2, items2, N - 1, None)

    def loop3(j, _):
        own(j, True)
        return 0

    lax.fori_loop(N - 1 - LAG, N - 1, loop3, 0)
    own(N - 1, False)

    parts[me] = acc[...]

    def part(k):
        to = lax.rem(me + k, DEVICES)
        return rcopy(acc, parts.at[me], psend, precv.at[k - 1], to)

    def part_in(k):
        frm = lax.rem(me + DEVICES - k, DEVICES)
        return rcopy(acc, parts.at[frm], psend, precv.at[k - 1], me)

    for k in range(1, DEVICES):
        part(k).start()
    for i in range(N - SLOTS, N):
        for cp in sends(2, i):
            cp.wait_send()
    wait_all(wa)
    for k in range(1, DEVICES):
        part_in(k).wait_recv()
    total = jnp.sum(jnp.sum(parts[...], axis=0))
    norm = jnp.sqrt(jnp.full((8, LANES), total, jnp.float32))
    nv[...] = norm
    norm_copy = pltpu.make_async_copy(nv, n_out, norm_sem)
    norm_copy.start()
    lr = lr_in[0]
    scale = jnp.minimum(1.0, jnp.full((8, LANES), clip_in[0], jnp.float32) / norm)

    def update(chunk):
        def group(k, _):
            rows = pl.ds(pl.multiple_of(chunk * R + k * GROUP, 8), GROUP)
            shape = (GROUP // 8, 8, LANES)
            h = gv[rows].reshape(shape) * scale[None]
            a = av[rows].reshape(shape) + h * h
            w = wv[rows].reshape(shape) - lr * h / (jnp.sqrt(a) + EPS)
            av[rows] = a.reshape(GROUP, LANES)
            wv[rows] = w.reshape(GROUP, LANES)
            return 0

        lax.fori_loop(0, R // GROUP, group, 0)

    def place(half, i, last):
        cut = OVER if (last and half == 1) else 0
        size = R - cut
        return pl.ds((half * N + i) * R + cut, size), (half * N + i) * R, size

    def f_rows(blk, half, i, last):
        _, lo, size = place(half, i, last)
        return pl.ds(blk * BLOCK + lo, size)

    def direct(link, which, blk, half, i, last):
        v, _, _ = place(half, i, last)
        rows = f_rows(blk, half, i, last)
        sem = recvx if link == 0 else recvy
        return rcopy(wv.at[v], full.at[rows], agsend.at[link, which], sem.at[which, i], nx if link == 0 else ny)

    def passed(link, blk, half, i, last):
        rows = f_rows(blk, half, i, last)
        sem = recvx if link == 0 else recvy
        return rcopy(full.at[rows], full.at[rows], agsend.at[link, 1], sem.at[1, i], nx if link == 0 else ny)

    def share(src, rows, k):
        return rcopy(src, full.at[rows], agd_send.at[k], agd_recv.at[k], mate)

    def emit(i, last):
        update(i)
        direct(0, 0, me, 0, i, last).start()
        update(N + i)
        direct(1, 0, me, 1, i, last).start()
        for half in (0, 1):
            v, lo, size = place(half, i, last)
            rows = f_rows(me, half, i, last)
            share(wv.at[v], rows, 0).start()
            pltpu.make_async_copy(wv.at[v], full.at[rows], loc_sem.at[0]).start()
            pltpu.make_async_copy(wv.at[v], w_out.at[pl.ds(lo, size)], loc_sem.at[1]).start()
            pltpu.make_async_copy(av.at[v], a_out.at[pl.ds(lo, size)], loc_sem.at[2]).start()

    def each(fn):
        def loop(i, _):
            fn(i, False)
            return 0

        lax.fori_loop(0, N - 1, loop, 0)
        fn(N - 1, True)

    each(emit)
    late = []
    for k, (row_x, row_y, size) in enumerate(list(piece_rows())[1:]):
        for q, (dst, row) in enumerate(((late_x[k], row_x), (late_y[k], row_y))):
            rows = pl.ds(row - MARGIN, size + 2 * MARGIN)
            late.append(pltpu.make_async_copy(wv.at[rows], dst, late_sem.at[k, q]))
    start_all(late)

    def forward(i, last):
        direct(0, 0, nx, 0, i, last).wait_recv()
        rows = f_rows(nx, 0, i, last)
        passed(1, nx, 0, i, last).start()
        share(full.at[rows], rows, 1).start()
        direct(1, 0, ny, 1, i, last).wait_recv()
        rows = f_rows(ny, 1, i, last)
        passed(0, ny, 1, i, last).start()
        share(full.at[rows], rows, 2).start()

    each(forward)

    direct(0, 2, me, 1, N - 1, True).start()
    direct(1, 2, me, 0, 0, False).start()

    def loop4(i, _):
        direct(0, 2, me, 1, i, False).start()
        direct(1, 2, me, 0, i - LATE, False).start()
        return 0

    lax.fori_loop(LATE + 1, N - 1, loop4, 0)
    row_x, row_y, size = list(piece_rows())[0]
    tails = [rcopy(wv.at[pl.ds(row_x - MARGIN, size + 2 * MARGIN)], tail_x, tail_sem.at[0, 0], tail_sem.at[0, 1], nx),
             rcopy(wv.at[pl.ds(row_y - MARGIN, size + 2 * MARGIN)], tail_y, tail_sem.at[1, 0], tail_sem.at[1, 1], ny)]
    start_all(tails)

    def take_passed(i, last):
        passed(1, nd, 0, i, last).wait_recv()
        rows = f_rows(nd, 0, i, last)
        share(full.at[rows], rows, 3).start()
        passed(0, nd, 1, i, last).wait_recv()
        rows = f_rows(nd, 1, i, last)
        share(full.at[rows], rows, 3).start()

    each(take_passed)

    def take_second(i, j, last):
        direct(0, 2, nx, 1, i, last).wait_recv()
        rows = f_rows(nx, 1, i, last)
        share(full.at[rows], rows, 1).start()
        direct(1, 2, ny, 0, j, False).wait_recv()
        rows = f_rows(ny, 0, j, False)
        share(full.at[rows], rows, 2).start()

    take_second(N - 1, 0, True)

    def loop5(i, _):
        take_second(i, i - LATE, False)
        return 0

    lax.fori_loop(LATE + 1, N - 1, loop5, 0)

    every = pl.ds(0, 4 * BLOCK)
    rcopy(full.at[every], full.at[every], dsend, drecv.at[0], mate).wait_send()
    every = pl.ds(0, 8 * (DEVICES - 1))
    rcopy(wv.at[every], wv.at[every], psend, precv.at[0], mate).wait_send()
    for link, halves in ((0, (0, 1, 1)), (1, (1, 0, 0))):
        for which, half in enumerate(halves):
            rows = pl.ds(0, N * R - half * OVER - ((LATE + 1) * R if which == 2 else 0))
            rcopy(full.at[rows], full.at[rows], agsend.at[link, which], recvx.at[0, 0], mate).wait_send()
    whole = pl.ds(0, BLOCK)
    for k in range(3):
        pltpu.make_async_copy(full.at[whole], full.at[whole], loc_sem.at[k]).wait()
    wait_all(late)
    norm_copy.wait()
    for k in range(4):
        rows = pl.ds(0, BLOCK - ((LATE + 1) * R if k in (1, 2) else 0))
        cp = rcopy(full.at[rows], full.at[rows], agd_send.at[k], agd_recv.at[k], mate)
        cp.wait_send()
        cp.wait_recv()
    wait_all(tails)


def bulk_body(f_ref, w_ref, a_ref, n_ref, copy_ref, w_out, a_out, n_out):
    n_out[0] = jnp.max(n_ref[...])
    copy_ref[...] = f_ref[...].astype(jnp.bfloat16)
    w_out[...] = w_ref[...]
    a_out[...] = a_ref[...]


def bulk(full, w_new, a_new, norm):
    big, small = (BULK_ROWS, LANES), (BULK_ROWS // 8 + 8 - BULK_ROWS // 8 % 8, LANES)
    at = lambda i: (i, 0)
    specs = [pl.BlockSpec(big, at), pl.BlockSpec(small, at), pl.BlockSpec(small, at)]
    return pl.pallas_call(
        bulk_body,
        name="bulk",
        grid=(pl.cdiv(full.shape[0], BULK_ROWS),),
        out_shape=(
            jax.ShapeDtypeStruct(full.shape, jnp.bfloat16),
            jax.ShapeDtypeStruct(w_new.shape, w_new.dtype),
            jax.ShapeDtypeStruct(a_new.shape, a_new.dtype),
            jax.ShapeDtypeStruct((1,), norm.dtype),
        ),
        in_specs=specs + [pl.BlockSpec(memory_space=pltpu.VMEM)],
        out_specs=(*specs, pl.BlockSpec(memory_space=pltpu.SMEM)),
        compiler_params=pltpu.CompilerParams(vmem_limit_bytes=54_000_000),
        cost_estimate=pl.CostEstimate(flops=full.size, bytes_accessed=8 * full.size, transcendentals=0),
    )(full, w_new, a_new, norm)


def place_pieces(k, size):
    rows = size + MARGIN

    def kernel(_, px, py, mx_, my_, out, f32s, b16s, in_sem, out_sem):
        me = lax.axis_index("dp")
        c, x, y = lax.rem(me, 2), lax.rem(me // 2, 2), me // 4
        starts = list(piece_rows())[k]
        ins, outs = [], []
        for q, (src, cc, xx, yy, lo) in enumerate((
            (px, c, 1 - x, y, starts[0]), (py, c, x, 1 - y, starts[1]),
            (mx_, 1 - c, 1 - x, y, starts[0]), (my_, 1 - c, x, 1 - y, starts[1]),
        )):
            first = ((yy * 2 + xx) * 2 + cc) * BLOCK + lo
            shift = lax.rem(first, MARGIN)
            ins.append(pltpu.make_async_copy(src.at[pl.ds(MARGIN - shift, rows)], f32s.at[q], in_sem.at[q]))
            aligned = pl.multiple_of(first - shift, MARGIN)
            outs.append(pltpu.make_async_copy(b16s.at[q], out.at[pl.ds(aligned, rows)], out_sem.at[q]))
        for cp in ins:
            cp.start()
        for q in range(4):
            ins[q].wait()
            b16s[q] = f32s[q].astype(jnp.bfloat16)
            outs[q].start()
        for cp in outs:
            cp.wait()

    any_spec = pl.BlockSpec(memory_space=pl.ANY)

    def call(out, px, py, mx_, my_):
        return pl.pallas_call(
            kernel,
            out_shape=jax.ShapeDtypeStruct(out.shape, out.dtype),
            in_specs=[any_spec] * 5,
            out_specs=any_spec,
            input_output_aliases={0: 0},
            scratch_shapes=[
                pltpu.VMEM((4, rows, LANES), jnp.float32),
                pltpu.VMEM((4, rows, LANES), jnp.bfloat16),
                pltpu.SemaphoreType.DMA((4,)),
                pltpu.SemaphoreType.DMA((4,)),
            ],
            compiler_params=pltpu.CompilerParams(vmem_limit_bytes=32_000_000),
            cost_estimate=pl.CostEstimate(flops=10_000_000, bytes_accessed=6 * 4 * rows * LANES, transcendentals=0),
        )(out, px, py, mx_, my_)

    return call


def solution(mesh):
    def local_step(grad_row, param_blk, accum_blk, learn_rate, clip_max):
        rows = grad_row.shape[1] // LANES
        f32 = jnp.float32
        any_spec = pl.BlockSpec(memory_space=pl.ANY)
        dma = pltpu.SemaphoreType.DMA
        smem = pl.BlockSpec(memory_space=pltpu.SMEM)
        late = tuple(jax.ShapeDtypeStruct((size + 2 * MARGIN, LANES), f32) for size in PIECES)
        tail = jax.ShapeDtypeStruct((R + 2 * MARGIN, LANES), f32)
        full, w_new, a_new, norm, *late = pl.pallas_call(
            body,
            name="adagrad_exchange",
            out_shape=(
                jax.ShapeDtypeStruct((rows, LANES), f32),
                jax.ShapeDtypeStruct((BLOCK, LANES), f32),
                jax.ShapeDtypeStruct((BLOCK, LANES), f32),
                jax.ShapeDtypeStruct((8, LANES), f32),
            ) + late + late + (tail, tail),
            in_specs=[smem, smem, any_spec, any_spec, any_spec],
            out_specs=(any_spec,) * 4
            + (any_spec,) * (2 * len(PIECES) + 2),
            scratch_shapes=[
                pltpu.VMEM((2 * N * R, LANES), f32),
                pltpu.VMEM((2 * N * R, LANES), f32),
                pltpu.VMEM((2 * N * R, LANES), f32),
                pltpu.VMEM((3, N * R, LANES), f32),
                pltpu.VMEM((3, N * R, LANES), f32),
                pltpu.VMEM((2, 4, 2, R, LANES), f32),
                pltpu.VMEM((SLOTS, R, LANES), f32),
                pltpu.VMEM((SLOTS, R, LANES), f32),
                pltpu.VMEM((8, LANES), f32),
                pltpu.VMEM((DEVICES, 8, LANES), f32),
                dma((2, 2)), dma((2, 4, 2)), dma((SLOTS,)), dma((SLOTS,)),
                dma((3, N)), dma((3, N)), dma(()), dma((2 * N + 6,)),
                dma(()), dma((DEVICES - 1,)),
                dma((2, 3)), dma((4,)), dma((4,)), dma((3,)), dma((len(PIECES), 2)), dma((2, 2)),
                pltpu.VMEM((8, LANES), f32), dma(()),
            ],
            compiler_params=pltpu.CompilerParams(
                collective_id=0, has_side_effects=True, vmem_limit_bytes=64_000_000
            ),
        )(
            learn_rate.reshape(1),
            clip_max.reshape(1),
            grad_row.reshape(rows, LANES),
            param_blk.reshape(BLOCK, LANES),
            accum_blk.reshape(BLOCK, LANES),
        )

        def permute(v, bit):
            return lax.ppermute(v, "dp", [(k, k ^ bit) for k in range(DEVICES)])

        copy, w_new, a_new, norm = bulk(full, w_new, a_new, norm)
        for k, (_, _, size) in enumerate(piece_rows()):
            if k == 0:
                px, py = late[-2:]
            else:
                px = permute(late[k - 1], 2)
                py = permute(late[len(PIECES) + k - 1], 4)
            dx = permute(px, 1)
            dy = permute(py, 1)
            copy = place_pieces(k, size)(copy, px, py, dx, dy)
        return w_new.reshape(-1), a_new.reshape(-1), copy.reshape(-1), norm[0]

    return jax.shard_map(
        local_step, mesh=mesh,
        in_specs=(P("dp", None), P("dp"), P("dp"), P(), P()),
        out_specs=(P("dp"), P("dp"), P(), P()), check_vma=False,
    )
```

```python
import jax
import jax.numpy as jnp
from jax import lax
from jax.experimental import pallas as pl
from jax.experimental.pallas import tpu as pltpu
from jax.sharding import PartitionSpec as P


EPS = 1e-10
MESH = pl.DeviceIdType.MESH
DEVICES = 8
LANES = 128
N = 28
R = 280
BLOCK = 15669
OVER = 2 * N * R - BLOCK
SLOTS = 6
LAG = 6
STEPS = ((1, 2), (2, 4), (4, 8), (8, N))
PASS = 14
GROUP = 56
PIECES = (4480, 1120, 560)
LATE = sum(PIECES) // R
BULK_ROWS = 7936
MARGIN = 8


def body(lr_in, clip_in, grad, w_in, a_in, full, w_out, a_out, n_out, *rest):
    k = len(PIECES)
    exchange(lr_in, clip_in, grad, w_in, a_in, full, w_out, a_out, n_out, rest[:k], rest[k : 2 * k], *rest[2 * k :])


def piece_rows():
    yield (N + LATE) * R, (N - 1 - LATE) * R, R
    lo = 0
    for size in PIECES:
        yield N * R + lo, (N - LATE) * R + lo, size
        lo += size


def exchange(lr_in, clip_in, grad, w_in, a_in, full, w_out, a_out, n_out, late_x, late_y, tail_x, tail_y,
         wv, av, gv, rx, ry, stage, sx, sy, acc, parts, row,
         wa_sem, load_sem, sendx, sendy, recv0, recv1, recvx, recvy, dsend, drecv, psend, precv,
         agsend, pass_sem, second_sem, tail_sem, agd_send, agd_recv, loc_sem, nv):
    me = lax.axis_index("dp")
    c, x, y = lax.rem(me, 2), lax.rem(me // 2, 2), me // 4

    def dev(cc, xx, yy):
        return (yy * 2 + xx) * 2 + cc

    nx, ny, nd, mate = dev(c, 1 - x, y), dev(c, x, 1 - y), dev(c, 1 - x, 1 - y), dev(1 - c, x, y)
    mx, my, md = dev(1 - c, 1 - x, y), dev(1 - c, x, 1 - y), dev(1 - c, 1 - x, 1 - y)

    def rcopy(src, dst, ssem, rsem, to):
        return pltpu.make_async_remote_copy(src, dst, ssem, rsem, device_id=(to,), device_id_type=MESH)

    def slab(bank, q, s):
        return stage.at[bank, q // 2, pl.ds((q % 2 * 2 + s) * R, R)]

    def both(bank, q):
        return slab(bank, q, 0)[...] + slab(bank, q, 1)[...]

    def take(ref, rows, sem):
        pltpu.make_async_copy(ref.at[pl.ds(0, rows)], ref.at[pl.ds(0, rows)], sem).wait()

    for half in (0, 1):
        rows = pl.ds(nd * BLOCK + half * N * R, R)
        pltpu.make_async_copy(grad.at[rows], slab(0, half, 0), load_sem.at[0, 0]).start()
    barrier = pltpu.get_barrier_semaphore()
    for k in range(1, DEVICES):
        pl.semaphore_signal(barrier, inc=1, device_id=(lax.rem(me + k, DEVICES),), device_id_type=MESH)
    pl.semaphore_wait(barrier, DEVICES - 1)

    def start_row(half, i):
        if half == 0:
            return i * R
        return (N + i) * R - OVER * ((i + 1) // N)

    def d2d(blk, lo, size, k):
        rows = pl.ds(blk * BLOCK + lo, size)
        return rcopy(grad.at[rows], full.at[rows], dsend, drecv.at[k], mate)

    def d2d_head(blk, half):
        rows = pl.ds(blk * BLOCK + half * N * R, R)
        return rcopy(grad.at[rows], slab(0, half, 1), dsend, drecv.at[half], mate)

    def d2d_first(blk, half, g):
        lo, hi = STEPS[g]
        cut = OVER if (hi == N and half == 1) else 0
        return d2d(blk, (half * N + lo) * R, (hi - lo) * R - cut, 2 + 2 * g + half)

    def d2d_half(blk, half, k):
        return d2d(blk, half * N * R, N * R - half * OVER, 2 + 2 * len(STEPS) + k)

    for half in (0, 1):
        d2d_head(md, half).start()
    for g in range(len(STEPS)):
        for half in (0, 1):
            d2d_first(md, half, g).start()
    for blk, half, k in ((mx, 0, 0), (my, 1, 0), (mx, 1, 1), (my, 0, 1), (mate, 0, 1), (mate, 1, 1)):
        d2d_half(blk, half, k).start()

    def loads(items, group, i, bank):
        for k, (blk, half) in enumerate(items):
            rows = pl.ds(blk * BLOCK + start_row(half, i), R)
            q = 2 * group + k
            pltpu.make_async_copy(grad.at[rows], slab(bank, q, 0), load_sem.at[bank, group]).start()
            pltpu.make_async_copy(full.at[rows], slab(bank, q, 1), load_sem.at[bank, group]).start()

    def loaded(group, bank):
        take(full, 4 * R, load_sem.at[bank, group])

    def start_all(copies):
        for cp in copies:
            cp.start()

    def sends(phase, i):
        slot = lax.rem(phase * N + i, SLOTS)
        rows = pl.ds(pl.multiple_of(i * R, 8), R)
        semx, semy = ((recv0.at[0], recv0.at[1]), (recv1.at[0], recv1.at[1]), (recvx.at[i], recvy.at[i]))[phase]
        return (rcopy(sx.at[slot], rx.at[phase, rows], sendx.at[slot], semx, nx),
                rcopy(sy.at[slot], ry.at[phase, rows], sendy.at[slot], semy, ny))

    def free_slot(phase, i):
        def go():
            for cp in sends(phase, i):
                cp.wait_send()

        if phase == 0:
            pl.when(i >= SLOTS)(go)
        else:
            go()

    def step(phase, items, i, more):
        bank = lax.rem(i, 2)
        slot = lax.rem(phase * N + i, SLOTS)
        free_slot(phase, i)
        loaded(0, bank)
        if phase < 2:
            sx[slot] = both(bank, 0)
            sy[slot] = both(bank, 1)
        else:
            rows = pl.ds(pl.multiple_of(i * R, 8), R)
            sx[slot] = both(bank, 0) + ry[0, rows]
            sy[slot] = both(bank, 1) + rx[0, rows]
        start_all(sends(phase, i))
        if more is not None:
            more(i + 1)
            loads(items, 0, i + 1, lax.rem(i + 1, 2))

    items0 = ((nd, 0), (nd, 1))

    def arrived(i):
        for g, (lo, _) in enumerate(STEPS):
            @pl.when(i == lo)
            def _():
                d2d_first(nd, 0, g).wait_recv()
                d2d_first(nd, 1, g).wait_recv()

    take(full, 2 * R, load_sem.at[0, 0])
    head = sends(0, 0)
    for half, slots in ((0, sx), (1, sy)):
        d2d_head(nd, half).wait_recv()
        slots[0] = both(0, half)
        head[half].start()
    for half in (0, 1):
        d2d_first(nd, half, 0).wait_recv()
    loads(items0, 0, 1, 1)

    def loop0(i, _):
        step(0, items0, i, arrived)
        return 0

    lax.fori_loop(1, N - 1, loop0, 0)
    step(0, items0, N - 1, None)

    body_rows = (2 * N - 1) * R
    wa = []
    for src, dst in ((w_in, wv), (a_in, av)):
        wa.append(pltpu.make_async_copy(src.at[pl.ds(0, body_rows)], dst.at[pl.ds(0, body_rows)], wa_sem))
        wa.append(pltpu.make_async_copy(src.at[pl.ds(BLOCK - R, R)], dst.at[pl.ds(body_rows, R)], wa_sem))
    start_all(wa)

    items1 = ((nx, 0), (ny, 1))
    take(full, BLOCK, drecv.at[2 + 2 * len(STEPS)])
    loads(items1, 0, 0, 0)

    def loop1(i, _):
        step(1, items1, i, lambda i: None)
        return 0

    lax.fori_loop(0, N - 1, loop1, 0)
    step(1, items1, N - 1, None)

    items2 = ((nx, 1), (ny, 0))
    itemsm = ((me, 0), (me, 1))
    take(full, 2 * BLOCK, drecv.at[3 + 2 * len(STEPS)])
    loads(items2, 0, 0, 0)
    loads(itemsm, 1, 0, 0)
    take(full, N * R, recv0.at[0])
    take(full, N * R, recv0.at[1])
    acc[...] = jnp.zeros_like(acc)

    def own(j, more):
        bank = lax.rem(j, 2)
        rows = pl.ds(pl.multiple_of(j * R, 8), R)
        brows = pl.ds(pl.multiple_of((N + j) * R, 8), R)
        for cp in sends(2, j):
            cp.wait_recv()
        loaded(1, bank)
        if more:
            loads(itemsm, 1, j + 1, lax.rem(j + 1, 2))
        ga = (both(bank, 2) + rx[1, rows] + ry[2, rows]) * (1.0 / DEVICES)
        gv[rows] = ga
        sq = jnp.sum((ga * ga).reshape(R // 8, 8, LANES), axis=0)
        gb = (both(bank, 3) + ry[1, rows] + rx[2, rows]) * (1.0 / DEVICES)
        gv[brows] = gb
        skip = OVER * ((j + 1) // N)
        row = lax.broadcasted_iota(jnp.int32, (R, LANES), 0)
        gb = jnp.where(row >= skip, gb, 0.0)
        acc[...] += sq + jnp.sum((gb * gb).reshape(R // 8, 8, LANES), axis=0)

    def loop2(i, _):
        step(2, items2, i, lambda i: None)

        @pl.when(i == LAG)
        def _():
            take(full, N * R, recv1.at[0])
            take(full, N * R, recv1.at[1])

        @pl.when(i >= LAG)
        def _():
            own(i - LAG, True)

        return 0

    lax.fori_loop(0, N - 1, loop2, 0)
    step(2, items2, N - 1, None)

    def loop3(j, _):
        own(j, True)
        return 0

    lax.fori_loop(N - 1 - LAG, N - 1, loop3, 0)
    own(N - 1, False)

    row[...] = jnp.sum(acc[...], axis=0, keepdims=True)
    parts[pl.ds(me, 1)] = row[...]

    def part(k):
        to = lax.rem(me + k, DEVICES)
        return rcopy(row, parts.at[pl.ds(me, 1)], psend, precv, to)

    for k in range(1, DEVICES):
        part(k).start()
    for i in range(N - SLOTS, N):
        for cp in sends(2, i):
            cp.wait_send()
    take(full, 4 * N * R, wa_sem)
    take(full, DEVICES - 1, precv)
    total = jnp.sum(parts[...])
    norm = jnp.sqrt(jnp.full((8, LANES), total, jnp.float32))
    nv[...] = norm
    norm_copy = pltpu.make_async_copy(nv, n_out, loc_sem)
    norm_copy.start()
    lr = lr_in[0]
    scale = jnp.minimum(1.0, jnp.full((8, LANES), clip_in[0], jnp.float32) / norm)

    def update(chunk):
        def group(k, _):
            rows = pl.ds(pl.multiple_of(chunk * R + k * GROUP, 8), GROUP)
            shape = (GROUP // 8, 8, LANES)
            h = gv[rows].reshape(shape) * scale[None]
            a = av[rows].reshape(shape) + h * h
            w = wv[rows].reshape(shape) - lr * h / (jnp.sqrt(a) + EPS)
            av[rows] = a.reshape(GROUP, LANES)
            wv[rows] = w.reshape(GROUP, LANES)
            return 0

        lax.fori_loop(0, R // GROUP, group, 0)

    def place(half, i, last):
        cut = OVER if (last and half == 1) else 0
        size = R - cut
        return pl.ds((half * N + i) * R + cut, size), (half * N + i) * R, size

    def f_rows(blk, half, i, last):
        _, lo, size = place(half, i, last)
        return pl.ds(blk * BLOCK + lo, size)

    def direct(link, blk, half, i, last, sem=None):
        v, _, _ = place(half, i, last)
        rows = f_rows(blk, half, i, last)
        sem = (recvx if link == 0 else recvy).at[i] if sem is None else second_sem.at[link, sem]
        return rcopy(wv.at[v], full.at[rows], agsend, sem, nx if link == 0 else ny)

    def passed(link, blk, half, i, last):
        rows = f_rows(blk, half, i, last)
        return rcopy(full.at[rows], full.at[rows], agsend, pass_sem.at[link, i // PASS], nx if link == 0 else ny)

    def share(src, rows):
        return rcopy(src, full.at[rows], agd_send, agd_recv, mate)

    def emit(i, last):
        update(i)
        direct(0, me, 0, i, last).start()
        update(N + i)
        direct(1, me, 1, i, last).start()
        for half in (0, 1):
            v, lo, size = place(half, i, last)
            rows = f_rows(me, half, i, last)
            share(wv.at[v], rows).start()
            pltpu.make_async_copy(wv.at[v], full.at[rows], loc_sem).start()
            pltpu.make_async_copy(wv.at[v], w_out.at[pl.ds(lo, size)], loc_sem).start()
            pltpu.make_async_copy(av.at[v], a_out.at[pl.ds(lo, size)], loc_sem).start()

    def each(fn):
        def loop(i, _):
            fn(i, False)
            return 0

        lax.fori_loop(0, N - 1, loop, 0)
        fn(N - 1, True)

    each(emit)
    late = []
    for k, (row_x, row_y, size) in enumerate(list(piece_rows())[1:]):
        for dst, row in ((late_x[k], row_x), (late_y[k], row_y)):
            rows = pl.ds(row - MARGIN, size + 2 * MARGIN)
            late.append(pltpu.make_async_copy(wv.at[rows], dst, loc_sem))
    start_all(late)

    def forward(i, last):
        direct(0, nx, 0, i, last).wait_recv()
        rows = f_rows(nx, 0, i, last)
        passed(1, nx, 0, i, last).start()
        share(full.at[rows], rows).start()
        direct(1, ny, 1, i, last).wait_recv()
        rows = f_rows(ny, 1, i, last)
        passed(0, ny, 1, i, last).start()
        share(full.at[rows], rows).start()

    each(forward)

    direct(0, me, 1, N - 1, True, 0).start()
    direct(1, me, 0, 0, False, 0).start()

    def loop4(i, _):
        direct(0, me, 1, i, False, i - LATE).start()
        direct(1, me, 0, i - LATE, False, i - LATE).start()
        return 0

    lax.fori_loop(LATE + 1, N - 1, loop4, 0)
    row_x, row_y, size = list(piece_rows())[0]
    tails = [rcopy(wv.at[pl.ds(row_x - MARGIN, size + 2 * MARGIN)], tail_x, agsend, tail_sem.at[0], nx),
             rcopy(wv.at[pl.ds(row_y - MARGIN, size + 2 * MARGIN)], tail_y, agsend, tail_sem.at[1], ny)]
    start_all(tails)

    for g in range(N // PASS):
        for link, half in ((1, 0), (0, 1)):
            cut = OVER if (g == N // PASS - 1 and half == 1) else 0
            size = PASS * R - cut
            take(full, size, pass_sem.at[link, g])
            rows = pl.ds(nd * BLOCK + (half * N + g * PASS) * R, size)
            share(full.at[rows], rows).start()

    def take_second(i, j, last, sem):
        direct(0, nx, 1, i, last, sem).wait_recv()
        rows = f_rows(nx, 1, i, last)
        share(full.at[rows], rows).start()
        direct(1, ny, 0, j, False, sem).wait_recv()
        rows = f_rows(ny, 0, j, False)
        share(full.at[rows], rows).start()

    take_second(N - 1, 0, True, 0)

    def loop5(i, _):
        take_second(i, i - LATE, False, i - LATE)
        return 0

    lax.fori_loop(LATE + 1, N - 1, loop5, 0)

    take(full, 4 * BLOCK, dsend)
    take(full, DEVICES - 1, psend)
    moved = 4 * BLOCK - 2 * (LATE + 1) * R
    take(full, 3 * BLOCK + sum(2 * (size + 2 * MARGIN) for size in PIECES) + 8, loc_sem)
    take(full, moved, agd_send)
    take(full, moved, agd_recv)
    for cp in tails:
        cp.wait_recv()
    take(full, 2 * BLOCK + 2 * (N - LATE - 1) * R - OVER + 2 * (R + 2 * MARGIN), agsend)


def bulk_body(f_ref, w_ref, a_ref, n_ref, copy_ref, w_out, a_out, n_out):
    n_out[0] = jnp.max(n_ref[...])
    copy_ref[...] = f_ref[...].astype(jnp.bfloat16)
    w_out[...] = w_ref[...]
    a_out[...] = a_ref[...]


def bulk(full, w_new, a_new, norm):
    grid = pl.cdiv(full.shape[0], BULK_ROWS)
    big, small = (BULK_ROWS, LANES), (8 * pl.cdiv(w_new.shape[0], 8 * grid), LANES)
    at = lambda i: (i, 0)
    specs = [pl.BlockSpec(big, at), pl.BlockSpec(small, at), pl.BlockSpec(small, at)]
    return pl.pallas_call(
        bulk_body,
        name="bulk",
        grid=(grid,),
        out_shape=(
            jax.ShapeDtypeStruct(full.shape, jnp.bfloat16),
            jax.ShapeDtypeStruct(w_new.shape, w_new.dtype),
            jax.ShapeDtypeStruct(a_new.shape, a_new.dtype),
            jax.ShapeDtypeStruct((1,), norm.dtype),
        ),
        in_specs=specs + [pl.BlockSpec(memory_space=pltpu.VMEM)],
        out_specs=(*specs, pl.BlockSpec(memory_space=pltpu.SMEM)),
        compiler_params=pltpu.CompilerParams(vmem_limit_bytes=54_000_000),
        cost_estimate=pl.CostEstimate(flops=full.size, bytes_accessed=8 * full.size, transcendentals=0),
    )(full, w_new, a_new, norm)


def place_pieces(k, size):
    rows = size + MARGIN

    def kernel(_, px, py, mx_, my_, out, f32s, b16s, in_sem, out_sem):
        me = lax.axis_index("dp")
        c, x, y = lax.rem(me, 2), lax.rem(me // 2, 2), me // 4
        starts = list(piece_rows())[k]
        ins, outs = [], []
        for q, (src, cc, xx, yy, lo) in enumerate((
            (px, c, 1 - x, y, starts[0]), (py, c, x, 1 - y, starts[1]),
            (mx_, 1 - c, 1 - x, y, starts[0]), (my_, 1 - c, x, 1 - y, starts[1]),
        )):
            first = ((yy * 2 + xx) * 2 + cc) * BLOCK + lo
            shift = lax.rem(first, MARGIN)
            ins.append(pltpu.make_async_copy(src.at[pl.ds(MARGIN - shift, rows)], f32s.at[q], in_sem.at[q]))
            aligned = pl.multiple_of(first - shift, MARGIN)
            outs.append(pltpu.make_async_copy(b16s.at[q], out.at[pl.ds(aligned, rows)], out_sem.at[q]))
        for cp in ins:
            cp.start()
        for q in range(4):
            ins[q].wait()
            b16s[q] = f32s[q].astype(jnp.bfloat16)
            outs[q].start()
        for cp in outs:
            cp.wait()

    any_spec = pl.BlockSpec(memory_space=pl.ANY)

    def call(out, px, py, mx_, my_):
        return pl.pallas_call(
            kernel,
            out_shape=jax.ShapeDtypeStruct(out.shape, out.dtype),
            in_specs=[any_spec] * 5,
            out_specs=any_spec,
            input_output_aliases={0: 0},
            scratch_shapes=[
                pltpu.VMEM((4, rows, LANES), jnp.float32),
                pltpu.VMEM((4, rows, LANES), jnp.bfloat16),
                pltpu.SemaphoreType.DMA((4,)),
                pltpu.SemaphoreType.DMA((4,)),
            ],
            compiler_params=pltpu.CompilerParams(vmem_limit_bytes=32_000_000),
            cost_estimate=pl.CostEstimate(flops=10_000_000, bytes_accessed=6 * 4 * rows * LANES, transcendentals=0),
        )(out, px, py, mx_, my_)

    return call


def solution(mesh):
    def local_step(grad_row, param_blk, accum_blk, learn_rate, clip_max):
        rows = grad_row.shape[1] // LANES
        f32 = jnp.float32
        any_spec = pl.BlockSpec(memory_space=pl.ANY)
        dma = pltpu.SemaphoreType.DMA
        smem = pl.BlockSpec(memory_space=pltpu.SMEM)
        late = tuple(jax.ShapeDtypeStruct((size + 2 * MARGIN, LANES), f32) for size in PIECES)
        tail = jax.ShapeDtypeStruct((R + 2 * MARGIN, LANES), f32)
        full, w_new, a_new, norm, *late = pl.pallas_call(
            body,
            name="adagrad_exchange",
            out_shape=(
                jax.ShapeDtypeStruct((rows, LANES), f32),
                jax.ShapeDtypeStruct((BLOCK, LANES), f32),
                jax.ShapeDtypeStruct((BLOCK, LANES), f32),
                jax.ShapeDtypeStruct((8, LANES), f32),
            ) + late + late + (tail, tail),
            in_specs=[smem, smem, any_spec, any_spec, any_spec],
            out_specs=(any_spec,) * 4
            + (any_spec,) * (2 * len(PIECES) + 2),
            scratch_shapes=[
                pltpu.VMEM((2 * N * R, LANES), f32),
                pltpu.VMEM((2 * N * R, LANES), f32),
                pltpu.VMEM((2 * N * R, LANES), f32),
                pltpu.VMEM((3, N * R, LANES), f32),
                pltpu.VMEM((3, N * R, LANES), f32),
                pltpu.VMEM((2, 2, 4 * R, LANES), f32),
                pltpu.VMEM((SLOTS, R, LANES), f32),
                pltpu.VMEM((SLOTS, R, LANES), f32),
                pltpu.VMEM((8, LANES), f32),
                pltpu.VMEM((DEVICES, LANES), f32),
                pltpu.VMEM((1, LANES), f32),
                dma(()), dma((2, 2)), dma((SLOTS,)), dma((SLOTS,)),
                dma((2,)), dma((2,)), dma((N,)), dma((N,)), dma(()), dma((4 + 2 * len(STEPS),)), dma(()), dma(()),
                dma(()), dma((2, N // PASS)), dma((2, N - LATE - 1)), dma((2,)), dma(()), dma(()), dma(()),
                pltpu.VMEM((8, LANES), f32),
            ],
            compiler_params=pltpu.CompilerParams(
                collective_id=0, has_side_effects=True, vmem_limit_bytes=64_000_000
            ),
        )(
            learn_rate.reshape(1),
            clip_max.reshape(1),
            grad_row.reshape(rows, LANES),
            param_blk.reshape(BLOCK, LANES),
            accum_blk.reshape(BLOCK, LANES),
        )

        def permute(v, bit):
            return lax.ppermute(v, "dp", [(k, k ^ bit) for k in range(DEVICES)])

        copy, w_new, a_new, norm = bulk(full, w_new, a_new, norm)
        for k, (_, _, size) in enumerate(piece_rows()):
            if k == 0:
                px, py = late[-2:]
            else:
                px = permute(late[k - 1], 2)
                py = permute(late[len(PIECES) + k - 1], 4)
            dx = permute(px, 1)
            dy = permute(py, 1)
            copy = place_pieces(k, size)(copy, px, py, dx, dy)
        return w_new.reshape(-1), a_new.reshape(-1), copy.reshape(-1), norm[0]

    return jax.shard_map(
        local_step, mesh=mesh,
        in_specs=(P("dp", None), P("dp"), P("dp"), P(), P()),
        out_specs=(P("dp"), P("dp"), P(), P()), check_vma=False,
    )
```
